32 devices in a mesh: slab: 8 (over z, y), sub: 4 (over x, core).
Axes of the slice: x: 2, y: 2, z: 4, core: 2. Of those that a mesh axis runs over, the one named last changes fastest.
Arguments:
- right_side: float32 [16, 8, 1, 16, 128], P('slab', 'sub'), may hold values from -8 to 8
- blocks: float32 [16, 8, 1, 7, 128, 128], P('slab', 'sub'), may hold values from -2300 to 4500, as said below
- pattern: int32 [16, 8, 1, 7], P('slab', 'sub'), may hold values from 0 to 127, as said below
- aggregates: int32 [16, 8, 1, 128], P('slab', 'sub'), may hold values from 0 to 127
- coarse_inverse: float32 [1024, 1024], P(('slab', 'sub')), may hold values from -0.1 to 0.8, as said below
Outputs:
- solution: float32 [16, 8, 1, 16, 128], P('slab', 'sub')
- residual: float32 [16, 8, 1, 16, 128], P('slab', 'sub')
The draws below stay inside these ranges and needn't reach their ends.
Inputs may be any that keep to these rules, and one draw needn't show every extreme that they name: `blocks`: taken with pattern, the operator A is symmetric positive definite, and the line systems of the steps are diagonally dominant with positive diagonals. `pattern`: the 7 entries of block row b list, in some order, b itself and the numbers of its six neighbours along x, y and z; a neighbour outside the grid of 16 x 8 x 1 block is replaced by b itself. `coarse_inverse`: symmetric positive definite.
All inputs are finite; a program needn't handle non-finite values.
Results may differ from the reference program's by a relative error of at most 0.0003.
Values sent between devices are 32-bit elements; how exact they have to be, the bound alone decides.
A program may use at most 128 MiB of HBM per device.

```python
import math
import jax
import jax.numpy as jnp
from jax import lax

BS = 128
LY = 1
LZ = 2
NRHS = 16
NCS = 128
ITERS = 2
BX = 8
BZ = 16
NC = 1024


def slot_order(key):
    scores = jax.random.randint(key, (BZ, BX, LY, 7), 0, 1 << 20) * 8 + jnp.arange(7, dtype=jnp.int32)
    return jnp.argsort(scores, axis=-1).astype(jnp.int32)


def grid_positions():
    z_position = jnp.broadcast_to(jnp.arange(BZ, dtype=jnp.int32)[:, None, None], (BZ, BX, LY))
    x_position = jnp.broadcast_to(jnp.arange(BX, dtype=jnp.int32)[None, :, None], (BZ, BX, LY))
    y_position = jnp.broadcast_to(jnp.arange(LY, dtype=jnp.int32)[None, None, :], (BZ, BX, LY))
    return (z_position, x_position, y_position)


def natural_columns():
    z_position, x_position, y_position = grid_positions()
    own_number = (z_position * BX + x_position) * LY + y_position
    below_x = jnp.where(x_position > 0, own_number - LY, own_number)
    above_x = jnp.where(x_position < BX - 1, own_number + LY, own_number)
    below_y = jnp.where(y_position > 0, own_number - 1, own_number)
    above_y = jnp.where(y_position < LY - 1, own_number + 1, own_number)
    below_z = jnp.where(z_position > 0, own_number - BX * LY, own_number)
    above_z = jnp.where(z_position < BZ - 1, own_number + BX * LY, own_number)
    return jnp.stack([own_number, below_x, above_x, below_y, above_y, below_z, above_z], axis=-1)


def draw_pattern(key, part):
    order = slot_order(jax.random.fold_in(key, 5))
    return jnp.take_along_axis(natural_columns(), order, axis=-1).astype(jnp.int32)


def face_coupling(subkey, strength, present):
    noise = jax.random.uniform(subkey, (BZ, BX, LY, BS, BS), jnp.float32, -1.0, 1.0) / BS
    identity = jnp.eye(BS, dtype=jnp.float32)
    off_diagonal = 0.5 * (noise + jnp.swapaxes(noise, -1, -2)) * (1.0 - identity)
    row_weight = jnp.sum(jnp.abs(off_diagonal), axis=-1)
    coupling = off_diagonal + identity * (row_weight + 0.1)[..., None]
    return strength * present[..., None, None] * coupling


def shifted_lower(coupling, axis):
    widths = [(0, 0)] * coupling.ndim
    widths[axis] = (1, 0)
    padded = jnp.pad(coupling, widths)
    return lax_slice_front(padded, axis, coupling.shape[axis])


def lax_slice_front(array, axis, length):
    return jnp.take(array, jnp.arange(length), axis=axis)


def draw_blocks(key, part):
    strength_x, strength_y, strength_z = (8.0, 1.0, 500.0)
    mass_low, mass_high = (0.3, 3.0)
    order = slot_order(jax.random.fold_in(key, 5))
    subkeys = jax.random.split(jax.random.fold_in(key, 6), 4)
    z_position, x_position, y_position = grid_positions()
    coupling_x = face_coupling(subkeys[0], strength_x, (x_position < BX - 1).astype(jnp.float32))
    coupling_y = face_coupling(subkeys[1], strength_y, (y_position < LY - 1).astype(jnp.float32))
    coupling_z = face_coupling(subkeys[2], strength_z, (z_position < BZ - 1).astype(jnp.float32))
    lower_x = shifted_lower(coupling_x, 1)
    lower_y = shifted_lower(coupling_y, 2)
    lower_z = shifted_lower(coupling_z, 0)
    mass_terms = jnp.exp(jax.random.uniform(subkeys[3], (BZ, BX, LY, BS), jnp.float32, math.log(mass_low), math.log(mass_high)))
    identity = jnp.eye(BS, dtype=jnp.float32)
    diagonal_block = identity * mass_terms[..., None] + coupling_x + lower_x + coupling_y + lower_y + coupling_z + lower_z
    natural = jnp.stack([diagonal_block, -lower_x, -coupling_x, -lower_y, -coupling_y, -lower_z, -coupling_z], axis=3)
    return jnp.take_along_axis(natural, order[..., None, None], axis=3)


def draw_coarse_inverse(key, part):
    subkeys = jax.random.split(key, 2)
    mixing = jax.random.uniform(subkeys[0], (NC, NC), jnp.float32, -1.0, 1.0)
    gram = jnp.dot(mixing, mixing.T, precision=lax.Precision.HIGHEST, preferred_element_type=jnp.float32) / NC
    gram = 0.5 * (gram + gram.T)
    factor = jnp.exp(jax.random.uniform(subkeys[1], (NC,), jnp.float32, math.log(0.3), math.log(1.0)))
    identity = jnp.eye(NC, dtype=jnp.float32)
    matrix = 0.05 * (gram + identity * factor[:, None])
    return matrix


def draw_right_side(key, part):
    subkeys = jax.random.split(key, 1)
    shape = (BZ, BX, LY, NRHS, BS)
    return jax.random.truncated_normal(subkeys[0], -6.0, 6.0, shape, jnp.float32)


def touch_ends(result, key, low, high):
    shape = result.shape
    place = [jax.random.randint(jax.random.fold_in(key, axis), (), 0, shape[axis]) for axis in range(len(shape))]
    result = result.at[tuple(place)].set(low)
    longest = shape.index(max(shape))
    place[longest] = (place[longest] + 1) % shape[longest]
    return result.at[tuple(place)].set(high)


def setup_inputs(seed: int = 0) -> dict:
    streams_of = jax.random.split(jax.random.key(seed), 6)
    right_side = draw_right_side(jax.random.fold_in(streams_of[5], 71), 0)
    blocks = draw_blocks(jax.random.fold_in(streams_of[5], 71), 0)
    pattern = draw_pattern(jax.random.fold_in(streams_of[5], 71), 0)
    aggregates = touch_ends(jax.random.randint(streams_of[3], (BZ, BX, LY, BS), 0, NCS), jax.random.fold_in(streams_of[3], 1), 0, NCS - 1).astype(jnp.int32)
    coarse_inverse = draw_coarse_inverse(jax.random.fold_in(streams_of[5], 71), 0)
    return {"right_side": right_side, "blocks": blocks, "pattern": pattern, "aggregates": aggregates, "coarse_inverse": coarse_inverse}


HIGHEST = lax.Precision.HIGHEST


def apply_operator(vector, blocks, pattern):
    flat_vector = vector.reshape(BZ * BX * LY, NRHS, BS)

    def one_plane(inputs):
        block_plane, slot_plane = inputs
        nearby = flat_vector[slot_plane]
        return jnp.einsum("rsij,rskj->rki", block_plane, nearby, precision=HIGHEST, preferred_element_type=jnp.float32)

    planes = lax.map(one_plane, (blocks.reshape(BZ, BX * LY, 7, BS, BS), pattern.reshape(BZ, BX * LY, 7)))
    return planes.reshape(BZ, BX, LY, NRHS, BS)


def line_terms(blocks, pattern):
    diagonals = jnp.diagonal(blocks, axis1=-2, axis2=-1)
    z_position = jnp.arange(BZ).astype(jnp.int32)
    x_position = jnp.arange(BX).astype(jnp.int32)
    y_position = jnp.arange(LY).astype(jnp.int32)
    own_number = ((z_position[:, None, None] * BX + x_position[None, :, None]) * LY + y_position[None, None, :]).astype(jnp.int32)
    is_self = (pattern == own_number[..., None]).astype(jnp.float32)
    is_below = (pattern == (own_number - BX * LY)[..., None]).astype(jnp.float32)
    line_diagonal = jnp.sum(diagonals * is_self[..., None], axis=3)
    line_coupling = jnp.sum(diagonals * is_below[..., None], axis=3)
    return line_diagonal, line_coupling


def line_pivots(line_diagonal, line_coupling):
    def advance(previous, inputs):
        diagonal_now, coupling_now = inputs
        pivot = diagonal_now - coupling_now * coupling_now / previous
        return pivot, pivot

    start = jnp.ones(line_diagonal.shape[1:], jnp.float32)
    _, pivots = lax.scan(advance, start, (line_diagonal, line_coupling))
    return pivots


def line_solve(values, pivots, line_coupling):
    upper = jnp.concatenate([line_coupling[1:], jnp.zeros_like(line_coupling[:1])], axis=0)

    def forward(previous, inputs):
        source, pivot, coupling = inputs
        current = (source - coupling[:, :, None, :] * previous) / pivot[:, :, None, :]
        return current, current

    start = jnp.zeros(values.shape[1:], jnp.float32)
    _, eliminated = lax.scan(forward, start, (values, pivots, line_coupling))

    def backward(later_value, inputs):
        eliminated_now, pivot, coupling = inputs
        current = eliminated_now - (coupling / pivot)[:, :, None, :] * later_value
        return current, current

    _, solved = lax.scan(backward, start, (eliminated, pivots, upper), reverse=True)
    return solved


def coarse_apply(values, aggregates, coarse_inverse):
    layer = (jnp.arange(BZ) // LZ).astype(jnp.int32)
    aggregate_ids = (aggregates + layer[:, None, None, None] * NCS).reshape(-1).astype(jnp.int32)
    cell_rows = jnp.swapaxes(values, -1, -2).reshape(-1, NRHS)
    partial_sums = jax.ops.segment_sum(cell_rows, aggregate_ids, num_segments=NC)
    coarse_values = jnp.dot(coarse_inverse, partial_sums, precision=HIGHEST, preferred_element_type=jnp.float32)
    returned = coarse_values[aggregate_ids].reshape(BZ, BX, LY, BS, NRHS)
    return jnp.swapaxes(returned, -1, -2)


def inner_product(left, right):
    return jnp.sum(left * right, axis=(0, 1, 2, 4))


def reference(right_side, blocks, pattern, aggregates, coarse_inverse):
    line_diagonal, line_coupling = line_terms(blocks, pattern)
    pivots = line_pivots(line_diagonal, line_coupling)

    def precondition(values):
        return line_solve(values, pivots, line_coupling) + coarse_apply(values, aggregates, coarse_inverse)

    solution = jnp.zeros_like(right_side)
    residual = right_side
    smoothed = precondition(residual)
    direction = smoothed
    energy = inner_product(residual, smoothed)
    for iteration in range(ITERS):
        applied = apply_operator(direction, blocks, pattern)
        step_length = energy / inner_product(direction, applied)
        solution = solution + step_length[:, None] * direction
        residual = residual - step_length[:, None] * applied
        if iteration + 1 < ITERS:
            smoothed = precondition(residual)
            energy_next = inner_product(residual, smoothed)
            direction = smoothed + (energy_next / energy)[:, None] * direction
            energy = energy_next
    return solution, residual
```

```python
import functools
import jax
import jax.numpy as jnp
from jax import lax
from jax.experimental import pallas as pl
from jax.experimental.pallas import tpu as pltpu
from jax.sharding import PartitionSpec as P

HIGHEST = lax.Precision.HIGHEST
MESH = pl.DeviceIdType.MESH
F32 = jnp.float32


def dot_nt(left, right):
    return lax.dot_general(
        left, right, (((1,), (1,)), ((), ())), precision=HIGHEST, preferred_element_type=F32
    )


def dot_nn(left, right):
    return lax.dot_general(
        left, right, (((1,), (0,)), ((), ())), precision=HIGHEST, preferred_element_type=F32
    )


def kernel(
    n_slab, n_sub, pattern, rhs, blocks, agg, inverse, sol, res,
    lines_r, lines_w, coefs, factors, solved, sub_a, sub_c, sub_e, slab_a, slab_c, slab_e,
    inv_all, halo_0, halo_1, applied_0, onehot,
    line_send, line_recv, coef_send, coef_recv, inv_send, inv_recv,
    sub_send, sub_recv, slab_send, slab_recv, halo_send, halo_recv,
):
    D, X, S, K, C = rhs.shape
    slots = blocks.shape[3]
    aggregates = inv_all.shape[0] * inv_all.shape[1]
    slab, sub = lax.axis_index("slab"), lax.axis_index("sub")
    cells = [(x, s) for x in range(X) for s in range(S)]
    rows = [(d, x, s) for d in range(D) for x, s in cells]
    width = len(cells)

    barrier = pltpu.get_barrier_semaphore()
    for step in range(1, n_slab):
        pl.semaphore_signal(
            barrier, inc=1, device_id=(lax.rem(slab + step, n_slab), sub), device_id_type=MESH
        )
    for step in range(1, n_sub):
        pl.semaphore_signal(
            barrier, inc=1, device_id=(slab, lax.rem(sub + step, n_sub)), device_id_type=MESH
        )

    def copies(axis, buffer, send, recv, source=None):
        count, mine = (n_slab, slab) if axis == "slab" else (n_sub, sub)
        made = []
        for step in range(1, count):
            peer = lax.rem(mine + step, count)
            target = (peer, sub) if axis == "slab" else (slab, peer)
            made.append(
                pltpu.make_async_remote_copy(
                    src_ref=buffer.at[mine] if source is None else source,
                    dst_ref=buffer.at[mine],
                    send_sem=send.at[step],
                    recv_sem=recv.at[mine],
                    device_id=target,
                    device_id_type=MESH,
                )
            )
        for copy in made:
            copy.start()

        def wait():
            for step in range(1, count):
                peer = lax.rem(mine + step, count)
                pltpu.make_async_remote_copy(
                    src_ref=buffer.at[peer],
                    dst_ref=buffer.at[peer],
                    send_sem=send.at[step],
                    recv_sem=recv.at[peer],
                    device_id=(peer, sub) if axis == "slab" else (slab, peer),
                    device_id_type=MESH,
                ).wait_recv()
            for copy in made:
                copy.wait_send()

        return wait

    a_index = lax.broadcasted_iota(jnp.int32, (aggregates, C), 0)
    for n, (d, x, s) in enumerate(rows):
        onehot[n] = (agg[d, x, s][None, :] == a_index).astype(F32)

    def local_sums(read):
        total = jnp.zeros((K, aggregates), F32)
        for n, (d, x, s) in enumerate(rows):
            total = total + dot_nt(read(d, x, s), onehot[n])
        return total

    sub_a[sub] = local_sums(lambda d, x, s: rhs[d, x, s])
    lines_r[slab] = rhs[...]
    inv_all[sub] = inverse[...]

    global_cross = X * n_sub
    plane_blocks = global_cross * S
    eye = (
        lax.broadcasted_iota(jnp.int32, (C, C), 0) == lax.broadcasted_iota(jnp.int32, (C, C), 1)
    ).astype(F32)
    for n, (d, x, s) in enumerate(rows):
        own = ((slab * D + d) * global_cross + sub * X + x) * S + s
        diagonal = jnp.zeros((C, C), F32)
        coupling = jnp.zeros((C, C), F32)
        for slot in range(slots):
            number = pattern[n * slots + slot]
            block = blocks[d, x, s, slot]
            diagonal = diagonal + (number == own).astype(F32) * block
            coupling = coupling + (number == own - plane_blocks).astype(F32) * block
        coefs[slab, pl.ds(n, 1)] = jnp.sum(diagonal * eye, axis=0, keepdims=True)
        coefs[slab, pl.ds(len(rows) + n, 1)] = jnp.sum(coupling * eye, axis=0, keepdims=True)

    pl.semaphore_wait(barrier, n_slab + n_sub - 2)

    sums_wait = copies("sub", sub_a, sub_send.at[0], sub_recv.at[0])
    coefs_wait = copies("slab", coefs, coef_send, coef_recv)
    lines_wait = copies("slab", lines_r, line_send.at[0], line_recv.at[0], rhs)
    inv_wait = copies("sub", inv_all, inv_send, inv_recv, inverse)

    sums_wait()
    total = sub_a[0]
    for other in range(1, n_sub):
        total = total + sub_a[other]
    slab_a[slab] = total
    slab_wait = copies("slab", slab_a, slab_send.at[0], slab_recv.at[0])

    coefs_wait()
    planes = n_slab * D

    def coef(kind, z):
        start = kind * len(rows) + (z % D) * width
        return coefs[z // D, pl.ds(start, width)]

    pivot = coef(0, 0)
    for z in range(planes):
        if z > 0:
            below = coef(1, z)
            pivot = coef(0, z) - below * below / pivot
        inverse_pivot = 1.0 / pivot
        factors[z, 0] = inverse_pivot
        factors[z, 1] = -coef(1, z) * inverse_pivot
        if z + 1 < planes:
            factors[z, 2] = -coef(1, z + 1) * inverse_pivot

    def line_solve(read):
        carried = [None] * width
        for z in range(planes):
            for w, (x, s) in enumerate(cells):
                value = read(z // D, z % D, x, s) * factors[z, 0, pl.ds(w, 1)]
                if z > 0:
                    value = value + factors[z, 1, pl.ds(w, 1)] * carried[w]
                carried[w] = value
                solved[z, x, s] = value
        for z in reversed(range(planes - 1)):
            for w, (x, s) in enumerate(cells):
                carried[w] = solved[z, x, s] + factors[z, 2, pl.ds(w, 1)] * carried[w]
                solved[z, x, s] = carried[w]

    def coarse(read):
        layer_rows = inv_all.shape[0] * inv_all.shape[1]
        values = jnp.zeros((K, layer_rows), F32)
        for layer in range(n_slab):
            piece = inv_all[:, :, pl.ds(layer * aggregates, aggregates)]
            values = values + dot_nt(read(layer), piece.reshape(layer_rows, aggregates))
        return values

    def smooth(halo, values):
        for n, (d, x, s) in enumerate(rows):
            halo[d + 1, x + 1, s] = solved[slab * D + d, x, s] + dot_nn(values, onehot[n])

    def exchange(halo, phase):
        def sides():
            inner_x, inner_z = pl.ds(1, X), pl.ds(1, D)
            return (
                (slab > 0, (slab - 1, sub), halo.at[1, inner_x], halo.at[D + 1, inner_x]),
                (slab < n_slab - 1, (slab + 1, sub), halo.at[D, inner_x], halo.at[0, inner_x]),
                (sub > 0, (slab, sub - 1), halo.at[inner_z, 1], halo.at[inner_z, X + 1]),
                (sub < n_sub - 1, (slab, sub + 1), halo.at[inner_z, X], halo.at[inner_z, 0]),
            )

        for side, (present, target, source, place) in enumerate(sides()):
            @pl.when(present)
            def _(side=side, target=target, source=source, place=place):
                pltpu.make_async_remote_copy(
                    src_ref=source, dst_ref=place,
                    send_sem=halo_send.at[phase, side], recv_sem=halo_recv.at[phase, side],
                    device_id=target, device_id_type=MESH,
                ).start()

        for side, (present, target, source, place) in enumerate(sides()):
            landing = sides()[side ^ 1][3]

            @pl.when(present)
            def _(side=side, target=target, source=source, landing=landing):
                pltpu.make_async_remote_copy(
                    src_ref=source, dst_ref=landing,
                    send_sem=halo_send.at[phase, side], recv_sem=halo_recv.at[phase, side ^ 1],
                    device_id=target, device_id_type=MESH,
                ).wait()

    def apply_operator(halo, n):
        total = jnp.zeros((K, C), F32)
        d, x, s = rows[n]
        for slot in range(slots):
            number = pattern[n * slots + slot]
            remain = number % plane_blocks
            local_plane = jnp.clip(number // plane_blocks - slab * D + 1, 0, D + 1)
            local_cross = jnp.clip(remain // S - sub * X + 1, 0, X + 1)
            total = total + dot_nt(halo[local_plane, local_cross, remain % S], blocks[d, x, s, slot])
        return total

    lane = lax.broadcasted_iota(jnp.int32, (K, C), 1)
    place = lax.broadcasted_iota(jnp.int32, (K, C), 0)

    def to_row(first, second):
        first = jnp.sum(first, axis=1, keepdims=True)
        second = jnp.sum(second, axis=1, keepdims=True)
        spread = jnp.where(lane == place, first, 0.0) + jnp.where(lane == place + K, second, 0.0)
        return jnp.sum(spread, axis=0, keepdims=True)

    def from_row(row):
        first = jnp.sum(jnp.where(lane == place, row, 0.0), axis=1, keepdims=True)
        second = jnp.sum(jnp.where(lane == place + K, row, 0.0), axis=1, keepdims=True)
        return first, second

    lines_wait()
    line_solve(lambda block, d, x, s: lines_r[block, d, x, s])
    slab_wait()
    inv_wait()
    smooth(halo_0, coarse(lambda layer: slab_a[layer]))

    exchange(halo_0, 0)
    energy = jnp.zeros((K, C), F32)
    curvature = jnp.zeros((K, C), F32)
    for n, (d, x, s) in enumerate(rows):
        applied = apply_operator(halo_0, n)
        lines_w[slab, d, x, s] = applied
        applied_0[d, x, s] = applied
        smoothed = halo_0[d + 1, x + 1, s]
        energy = energy + rhs[d, x, s] * smoothed
        curvature = curvature + applied * smoothed

    sub_c[sub, pl.ds(0, K)] = local_sums(lambda d, x, s: applied_0[d, x, s])
    sub_c[sub, pl.ds(K, 1)] = to_row(energy, curvature)
    sums_wait = copies("sub", sub_c, sub_send.at[1], sub_recv.at[1])
    lines_wait = copies("slab", lines_w, line_send.at[1], line_recv.at[1])
    sums_wait()
    total = sub_c[0]
    for other in range(1, n_sub):
        total = total + sub_c[other]
    slab_c[slab] = total
    slab_wait = copies("slab", slab_c, slab_send.at[1], slab_recv.at[1])
    slab_wait()
    row = slab_c[0, pl.ds(K, 1)]
    for other in range(1, n_slab):
        row = row + slab_c[other, pl.ds(K, 1)]
    energy, curvature = from_row(row)
    step_length = energy / curvature
    values = coarse(lambda layer: slab_a[layer] - step_length * slab_c[layer, pl.ds(0, K)])
    lines_wait()
    line_solve(
        lambda block, d, x, s: lines_r[block, d, x, s] - step_length * lines_w[block, d, x, s]
    )
    smooth(halo_1, values)

    exchange(halo_1, 1)
    energy_sum = jnp.zeros((K, C), F32)
    curvature_sum = jnp.zeros((K, C), F32)
    for n, (d, x, s) in enumerate(rows):
        applied = apply_operator(halo_1, n)
        sol[d, x, s] = applied
        smoothed = halo_1[d + 1, x + 1, s]
        residual = rhs[d, x, s] - step_length * applied_0[d, x, s]
        energy_sum = energy_sum + residual * smoothed
        curvature_sum = curvature_sum + applied * smoothed

    sub_e[sub] = to_row(energy_sum, curvature_sum)
    copies("sub", sub_e, sub_send.at[2], sub_recv.at[2])()
    row = sub_e[0]
    for other in range(1, n_sub):
        row = row + sub_e[other]
    slab_e[slab] = row
    copies("slab", slab_e, slab_send.at[2], slab_recv.at[2])()
    row = slab_e[0]
    for other in range(1, n_slab):
        row = row + slab_e[other]
    energy_next, curvature = from_row(row)
    growth = energy_next / energy
    step_next = energy_next / (curvature - growth * energy_next / step_length)
    for n, (d, x, s) in enumerate(rows):
        first, second = halo_0[d + 1, x + 1, s], halo_1[d + 1, x + 1, s]
        along_0, along_1 = applied_0[d, x, s], sol[d, x, s]
        residual = rhs[d, x, s] - step_length * along_0
        res[d, x, s] = residual - step_next * (along_1 + growth * along_0)
        sol[d, x, s] = step_length * first + step_next * (second + growth * first)


def per_device(n_slab, n_sub, right_side, blocks, pattern, aggregates, coarse_inverse):
    D, X, S, K, C = right_side.shape
    owned, everything = coarse_inverse.shape
    layer = owned * n_sub
    planes = n_slab * D
    packed = -(-(K + 1) // 8) * 8
    rows = D * X * S
    field = (D, X, S, K, C)
    halo = (D + 2, X + 2, S, K, C)
    dma = pltpu.SemaphoreType.DMA
    vmem = pl.BlockSpec(memory_space=pltpu.VMEM)
    return pl.pallas_call(
        functools.partial(kernel, n_slab, n_sub),
        out_shape=[jax.ShapeDtypeStruct(field, F32)] * 2,
        in_specs=[pl.BlockSpec(memory_space=pltpu.SMEM), vmem, vmem, vmem, vmem],
        out_specs=[vmem, vmem],
        scratch_shapes=[
            pltpu.VMEM((n_slab,) + field, F32),
            pltpu.VMEM((n_slab,) + field, F32),
            pltpu.VMEM((n_slab, 2 * rows, C), F32),
            pltpu.VMEM((planes, 3, X * S, C), F32),
            pltpu.VMEM((planes, X, S, K, C), F32),
            pltpu.VMEM((n_sub, K, layer), F32),
            pltpu.VMEM((n_sub, packed, layer), F32),
            pltpu.VMEM((n_sub, 1, C), F32),
            pltpu.VMEM((n_slab, K, layer), F32),
            pltpu.VMEM((n_slab, packed, layer), F32),
            pltpu.VMEM((n_slab, 1, C), F32),
            pltpu.VMEM((n_sub, owned, everything), F32),
            pltpu.VMEM(halo, F32),
            pltpu.VMEM(halo, F32),
            pltpu.VMEM(field, F32),
            pltpu.VMEM((rows, layer, C), F32),
            dma((2, n_slab)), dma((2, n_slab)),
            dma((n_slab,)), dma((n_slab,)),
            dma((n_sub,)), dma((n_sub,)),
            dma((3, n_sub)), dma((3, n_sub)),
            dma((3, n_slab)), dma((3, n_slab)),
            dma((2, 4)), dma((2, 4)),
        ],
        compiler_params=pltpu.CompilerParams(
            collective_id=0, has_side_effects=True, vmem_limit_bytes=60 * 1024 * 1024
        ),
        name="whole_solve",
    )(pattern.reshape(-1), right_side, blocks, aggregates, coarse_inverse)


def solution(mesh):
    placed = (
        P("slab", "sub", None, None, None),
        P("slab", "sub", None, None, None, None),
        P("slab", "sub", None, None),
        P("slab", "sub", None, None),
        P(("slab", "sub"), None),
    )
    body = functools.partial(per_device, mesh.shape["slab"], mesh.shape["sub"])
    return jax.shard_map(
        lambda *args: tuple(body(*args)),
        mesh=mesh,
        in_specs=placed,
        out_specs=(P("slab", "sub", None, None, None), P("slab", "sub", None, None, None)),
        check_vma=False,
    )
```

```python
import functools
import jax
import jax.numpy as jnp
from jax import lax
from jax.experimental import pallas as pl
from jax.experimental.pallas import tpu as pltpu
from jax.sharding import PartitionSpec as P

MESH = pl.DeviceIdType.MESH
F32 = jnp.float32
BF16 = jnp.bfloat16


def dot(left, right, right_dim):
    return lax.dot_general(
        left, right, (((1,), (right_dim,)), ((), ())), preferred_element_type=F32
    )


def pieces(value, count, axis=0):
    parts = []
    for _ in range(count):
        part = value.astype(BF16)
        parts.append(part)
        value = value - part.astype(F32)
    return jnp.concatenate(parts, axis=axis)


def joined(product):
    height, half = product.shape[0] // 3, product.shape[1] // 2
    high, mid, low = (product[n * height : (n + 1) * height] for n in range(3))
    small = low[:, :half] + mid[:, half:] + low[:, half:]
    return small + (mid[:, :half] + high[:, half:]) + high[:, :half]


def stacked(product):
    height = product.shape[0] // 3
    return (product[2 * height :] + product[height : 2 * height]) + product[:height]


def kernel(
    n_slab, n_sub, pattern, rhs, blocks, agg, inverse, sol, res,
    lines_r, lines_w, coefs, factors, solved, sub_a, sub_c, sub_e, slab_a, slab_c, slab_e,
    inv_all, halo_0, halo_1, applied_0, onehot,
    block_here, block_split, inv_split, halo_split, block_sem,
    line_send, line_recv, coef_send, coef_recv, inv_send, inv_recv,
    sub_send, sub_recv, slab_send, slab_recv, halo_send, halo_recv,
):
    D, X, S, K, C = rhs.shape
    block_copy = pltpu.make_async_copy(blocks, block_here, block_sem)
    block_copy.start()
    slots = blocks.shape[3]
    aggregates = inv_all.shape[0] * inv_all.shape[1]
    slab, sub = lax.axis_index("slab"), lax.axis_index("sub")
    cells = [(x, s) for x in range(X) for s in range(S)]
    rows = [(d, x, s) for d in range(D) for x, s in cells]
    width = len(cells)

    barrier = pltpu.get_barrier_semaphore()
    for step in range(1, n_slab):
        pl.semaphore_signal(
            barrier, inc=1, device_id=(lax.rem(slab + step, n_slab), sub), device_id_type=MESH
        )
    for step in range(1, n_sub):
        pl.semaphore_signal(
            barrier, inc=1, device_id=(slab, lax.rem(sub + step, n_sub)), device_id_type=MESH
        )

    def copies(axis, buffer, send, recv, source=None):
        count, mine = (n_slab, slab) if axis == "slab" else (n_sub, sub)
        made = []
        for step in range(1, count):
            peer = lax.rem(mine + step, count)
            target = (peer, sub) if axis == "slab" else (slab, peer)
            made.append(
                pltpu.make_async_remote_copy(
                    src_ref=buffer.at[mine] if source is None else source,
                    dst_ref=buffer.at[mine],
                    send_sem=send.at[step],
                    recv_sem=recv.at[mine],
                    device_id=target,
                    device_id_type=MESH,
                )
            )
        for copy in made:
            copy.start()

        def wait():
            for step in range(1, count):
                peer = lax.rem(mine + step, count)
                pltpu.make_async_remote_copy(
                    src_ref=buffer.at[peer],
                    dst_ref=buffer.at[peer],
                    send_sem=send.at[step],
                    recv_sem=recv.at[peer],
                    device_id=(peer, sub) if axis == "slab" else (slab, peer),
                    device_id_type=MESH,
                ).wait_recv()
            for copy in made:
                copy.wait_send()

        return wait

    a_index = lax.broadcasted_iota(jnp.int32, (aggregates, C), 0)
    for n, (d, x, s) in enumerate(rows):
        onehot[:, pl.ds(n * C, C)] = (agg[d, x, s][None, :] == a_index).astype(F32).astype(BF16)

    def local_sums(read):
        split = jnp.concatenate([pieces(read(d, x, s), 3) for d, x, s in rows], axis=1)
        return stacked(dot(split, onehot[...], 1))

    sub_a[sub] = local_sums(lambda d, x, s: rhs[d, x, s])
    lines_r[slab] = rhs[...]
    inv_all[sub] = inverse[...]

    global_cross = X * n_sub
    plane_blocks = global_cross * S
    block_copy.wait()
    eye = (
        lax.broadcasted_iota(jnp.int32, (C, C), 0) == lax.broadcasted_iota(jnp.int32, (C, C), 1)
    ).astype(F32)
    for n, (d, x, s) in enumerate(rows):
        own = ((slab * D + d) * global_cross + sub * X + x) * S + s
        diagonal = jnp.zeros((C, C), F32)
        coupling = jnp.zeros((C, C), F32)
        for slot in range(slots):
            number = pattern[d, x, s, slot]
            block = block_here[d, x, s, slot]
            diagonal = diagonal + (number == own).astype(F32) * block
            coupling = coupling + (number == own - plane_blocks).astype(F32) * block
        coefs[slab, pl.ds(n, 1)] = jnp.sum(diagonal * eye, axis=0, keepdims=True)
        coefs[slab, pl.ds(len(rows) + n, 1)] = jnp.sum(coupling * eye, axis=0, keepdims=True)

    pl.semaphore_wait(barrier, n_slab + n_sub - 2)

    sums_wait = copies("sub", sub_a, sub_send.at[0], sub_recv.at[0])
    coefs_wait = copies("slab", coefs, coef_send, coef_recv)
    lines_wait = copies("slab", lines_r, line_send.at[0], line_recv.at[0], rhs)
    inv_wait = copies("sub", inv_all, inv_send, inv_recv, inverse)

    sums_wait()
    total = sub_a[0]
    for other in range(1, n_sub):
        total = total + sub_a[other]
    slab_a[slab] = total
    slab_wait = copies("slab", slab_a, slab_send.at[0], slab_recv.at[0])

    coefs_wait()
    planes = n_slab * D

    def coef(kind, z):
        start = kind * len(rows) + (z % D) * width
        return coefs[z // D, pl.ds(start, width)]

    pivot = coef(0, 0)
    for z in range(planes):
        if z > 0:
            below = coef(1, z)
            pivot = coef(0, z) - below * below / pivot
        inverse_pivot = 1.0 / pivot
        factors[z, 0] = inverse_pivot
        factors[z, 1] = -coef(1, z) * inverse_pivot
        if z + 1 < planes:
            factors[z, 2] = -coef(1, z + 1) * inverse_pivot

    def line_solve(lines):
        carried = [None] * width
        for z in range(planes):
            for w, (x, s) in enumerate(cells):
                value = lines[z // D, z % D, x, s] * factors[z, 0, pl.ds(w, 1)]
                if z > 0:
                    value = value + factors[z, 1, pl.ds(w, 1)] * carried[w]
                carried[w] = value
                solved[z, x, s] = value
        for z in reversed(range(planes - 1)):
            for w, (x, s) in enumerate(cells):
                carried[w] = solved[z, x, s] + factors[z, 2, pl.ds(w, 1)] * carried[w]
                solved[z, x, s] = carried[w]

    def coarse(read):
        split = jnp.concatenate([pieces(read(layer), 3) for layer in range(n_slab)], axis=1)
        values = joined(dot(split, inv_split[...], 1))
        return stacked(dot(pieces(values, 3), onehot[...], 0))

    for n, (d, x, s) in enumerate(rows):
        for slot in range(slots):
            block_split[n, :, pl.ds(slot * C, C)] = pieces(block_here[d, x, s, slot], 2)

    def exchange(halo, phase):
        def sides():
            inner_x, inner_z = pl.ds(1, X), pl.ds(1, D)
            return (
                (slab > 0, (slab - 1, sub), halo.at[1, inner_x], halo.at[D + 1, inner_x]),
                (slab < n_slab - 1, (slab + 1, sub), halo.at[D, inner_x], halo.at[0, inner_x]),
                (sub > 0, (slab, sub - 1), halo.at[inner_z, 1], halo.at[inner_z, X + 1]),
                (sub < n_sub - 1, (slab, sub + 1), halo.at[inner_z, X], halo.at[inner_z, 0]),
            )

        for side, (present, target, source, place) in enumerate(sides()):
            @pl.when(present)
            def _(side=side, target=target, source=source, place=place):
                pltpu.make_async_remote_copy(
                    src_ref=source, dst_ref=place,
                    send_sem=halo_send.at[phase, side], recv_sem=halo_recv.at[phase, side],
                    device_id=target, device_id_type=MESH,
                ).start()

        for side, (present, target, source, place) in enumerate(sides()):
            landing = sides()[side ^ 1][3]

            @pl.when(present)
            def _(side=side, target=target, source=source, landing=landing):
                pltpu.make_async_remote_copy(
                    src_ref=source, dst_ref=landing,
                    send_sem=halo_send.at[phase, side], recv_sem=halo_recv.at[phase, side ^ 1],
                    device_id=target, device_id_type=MESH,
                ).wait()

    def split_halo(halo):
        for d in range(D + 2):
            for x in range(X + 2):
                if 0 < d <= D or 0 < x <= X:
                    for s in range(S):
                        halo_split[d, x, s] = pieces(halo[d, x, s], 3)

    def apply_operator(n):
        d, x, s = rows[n]
        nearby = []
        for slot in range(slots):
            number = pattern[d, x, s, slot]
            remain = number % plane_blocks
            local_plane = jnp.clip(number // plane_blocks - slab * D + 1, 0, D + 1)
            local_cross = jnp.clip(remain // S - sub * X + 1, 0, X + 1)
            nearby.append(halo_split[local_plane, local_cross, remain % S])
        return joined(dot(jnp.concatenate(nearby, axis=1), block_split[n], 1))

    lane = lax.broadcasted_iota(jnp.int32, (K, C), 1)
    place = lax.broadcasted_iota(jnp.int32, (K, C), 0)

    def to_row(first, second):
        first = jnp.sum(first, axis=1, keepdims=True)
        second = jnp.sum(second, axis=1, keepdims=True)
        spread = jnp.where(lane == place, first, 0.0) + jnp.where(lane == place + K, second, 0.0)
        return jnp.sum(spread, axis=0, keepdims=True)

    def from_row(row):
        first = jnp.sum(jnp.where(lane == place, row, 0.0), axis=1, keepdims=True)
        second = jnp.sum(jnp.where(lane == place + K, row, 0.0), axis=1, keepdims=True)
        return first, second

    inv_wait()
    for other in range(n_sub):
        owned = inv_all.shape[1]
        part = inv_all[other]
        high = part.astype(BF16)
        inv_split[pl.ds(other * owned, owned)] = high
        inv_split[pl.ds((n_sub + other) * owned, owned)] = (part - high.astype(F32)).astype(BF16)
    lines_wait()
    line_solve(lines_r)
    slab_wait()
    spread = coarse(lambda layer: slab_a[layer])
    for n, (d, x, s) in enumerate(rows):
        halo_0[d + 1, x + 1, s] = solved[slab * D + d, x, s] + spread[:, n * C : (n + 1) * C]

    exchange(halo_0, 0)
    split_halo(halo_0)
    energy = jnp.zeros((K, C), F32)
    curvature = jnp.zeros((K, C), F32)
    for n, (d, x, s) in enumerate(rows):
        applied = apply_operator(n)
        lines_w[slab, d, x, s] = applied
        applied_0[d, x, s] = applied
        smoothed = halo_0[d + 1, x + 1, s]
        energy = energy + rhs[d, x, s] * smoothed
        curvature = curvature + applied * smoothed

    sub_c[sub, pl.ds(0, K)] = local_sums(lambda d, x, s: applied_0[d, x, s])
    sub_c[sub, pl.ds(K, 1)] = to_row(energy, curvature)
    sums_wait = copies("sub", sub_c, sub_send.at[1], sub_recv.at[1])
    lines_wait = copies("slab", lines_w, line_send.at[1], line_recv.at[1])
    sums_wait()
    total = sub_c[0]
    for other in range(1, n_sub):
        total = total + sub_c[other]
    slab_c[slab] = total
    slab_wait = copies("slab", slab_c, slab_send.at[1], slab_recv.at[1])
    lines_wait()
    line_solve(lines_w)
    slab_wait()
    row = slab_c[0, pl.ds(K, 1)]
    for other in range(1, n_slab):
        row = row + slab_c[other, pl.ds(K, 1)]
    energy, curvature = from_row(row)
    step_length = energy / curvature
    spread = coarse(lambda layer: slab_c[layer, pl.ds(0, K)])
    for n, (d, x, s) in enumerate(rows):
        change = solved[slab * D + d, x, s] + spread[:, n * C : (n + 1) * C]
        halo_1[d + 1, x + 1, s] = halo_0[d + 1, x + 1, s] - step_length * change

    exchange(halo_1, 1)
    split_halo(halo_1)
    energy_sum = jnp.zeros((K, C), F32)
    curvature_sum = jnp.zeros((K, C), F32)
    for n, (d, x, s) in enumerate(rows):
        applied = apply_operator(n)
        sol[d, x, s] = applied
        smoothed = halo_1[d + 1, x + 1, s]
        residual = rhs[d, x, s] - step_length * applied_0[d, x, s]
        energy_sum = energy_sum + residual * smoothed
        curvature_sum = curvature_sum + applied * smoothed

    sub_e[sub] = to_row(energy_sum, curvature_sum)
    copies("sub", sub_e, sub_send.at[2], sub_recv.at[2])()
    row = sub_e[0]
    for other in range(1, n_sub):
        row = row + sub_e[other]
    slab_e[slab] = row
    copies("slab", slab_e, slab_send.at[2], slab_recv.at[2])()
    row = slab_e[0]
    for other in range(1, n_slab):
        row = row + slab_e[other]
    energy_next, curvature = from_row(row)
    growth = energy_next / energy
    step_next = energy_next / (curvature - growth * energy_next / step_length)
    for n, (d, x, s) in enumerate(rows):
        first, second = halo_0[d + 1, x + 1, s], halo_1[d + 1, x + 1, s]
        along_0, along_1 = applied_0[d, x, s], sol[d, x, s]
        residual = rhs[d, x, s] - step_length * along_0
        res[d, x, s] = residual - step_next * (along_1 + growth * along_0)
        sol[d, x, s] = step_length * first + step_next * (second + growth * first)


def per_device(n_slab, n_sub, right_side, blocks, pattern, aggregates, coarse_inverse):
    D, X, S, K, C = right_side.shape
    owned, everything = coarse_inverse.shape
    layer = owned * n_sub
    planes = n_slab * D
    packed = -(-(K + 1) // 8) * 8
    rows = D * X * S
    field = (D, X, S, K, C)
    halo = (D + 2, X + 2, S, K, C)
    dma = pltpu.SemaphoreType.DMA
    vmem = pl.BlockSpec(memory_space=pltpu.VMEM)
    return pl.pallas_call(
        functools.partial(kernel, n_slab, n_sub),
        out_shape=[jax.ShapeDtypeStruct(field, F32)] * 2,
        in_specs=[
            pl.BlockSpec(memory_space=pltpu.SMEM), vmem, pl.BlockSpec(memory_space=pl.ANY), vmem, vmem,
        ],
        out_specs=[vmem, vmem],
        scratch_shapes=[
            pltpu.VMEM((n_slab,) + field, F32),
            pltpu.VMEM((n_slab,) + field, F32),
            pltpu.VMEM((n_slab, 2 * rows, C), F32),
            pltpu.VMEM((planes, 3, X * S, C), F32),
            pltpu.VMEM((planes, X, S, K, C), F32),
            pltpu.VMEM((n_sub, K, layer), F32),
            pltpu.VMEM((n_sub, packed, layer), F32),
            pltpu.VMEM((n_sub, 1, C), F32),
            pltpu.VMEM((n_slab, K, layer), F32),
            pltpu.VMEM((n_slab, packed, layer), F32),
            pltpu.VMEM((n_slab, 1, C), F32),
            pltpu.VMEM((n_sub, owned, everything), F32),
            pltpu.VMEM(halo, F32),
            pltpu.VMEM(halo, F32),
            pltpu.VMEM(field, F32),
            pltpu.VMEM((layer, rows * C), BF16),
            pltpu.VMEM(blocks.shape, F32),
            pltpu.VMEM((rows, 2 * C, blocks.shape[3] * C), BF16),
            pltpu.VMEM((2 * layer, everything), BF16),
            pltpu.VMEM((D + 2, X + 2, S, 3 * K, C), BF16),
            dma,
            dma((2, n_slab)), dma((2, n_slab)),
            dma((n_slab,)), dma((n_slab,)),
            dma((n_sub,)), dma((n_sub,)),
            dma((3, n_sub)), dma((3, n_sub)),
            dma((3, n_slab)), dma((3, n_slab)),
            dma((2, 4)), dma((2, 4)),
        ],
        compiler_params=pltpu.CompilerParams(
            collective_id=0, has_side_effects=True, vmem_limit_bytes=60 * 1024 * 1024
        ),
        name="whole_solve",
    )(pattern, right_side, blocks, aggregates, coarse_inverse)


def solution(mesh):
    placed = (
        P("slab", "sub", None, None, None),
        P("slab", "sub", None, None, None, None),
        P("slab", "sub", None, None),
        P("slab", "sub", None, None),
        P(("slab", "sub"), None),
    )
    body = functools.partial(per_device, mesh.shape["slab"], mesh.shape["sub"])
    return jax.shard_map(
        lambda *args: tuple(body(*args)),
        mesh=mesh,
        in_specs=placed,
        out_specs=(P("slab", "sub", None, None, None), P("slab", "sub", None, None, None)),
        check_vma=False,
    )
```

```python
import functools
import jax
import jax.numpy as jnp
from jax import lax
from jax.experimental import pallas as pl
from jax.experimental.pallas import tpu as pltpu
from jax.sharding import PartitionSpec as P

MESH = pl.DeviceIdType.MESH
F32 = jnp.float32
BF16 = jnp.bfloat16


def dot(left, right, right_dim):
    return lax.dot_general(
        left, right, (((1,), (right_dim,)), ((), ())), preferred_element_type=F32
    )


def pieces(value, count, axis=0):
    parts = []
    for _ in range(count):
        part = value.astype(BF16)
        parts.append(part)
        value = value - part.astype(F32)
    return jnp.concatenate(parts, axis=axis)


def joined(product):
    height, half = product.shape[0] // 3, product.shape[1] // 2
    high, mid, low = (product[n * height : (n + 1) * height] for n in range(3))
    small = low[:, :half] + mid[:, half:] + low[:, half:]
    return small + (mid[:, :half] + high[:, half:]) + high[:, :half]


def stacked(product):
    height = product.shape[0] // 3
    return (product[2 * height :] + product[height : 2 * height]) + product[:height]


def kernel(
    n_slab, n_sub, pattern, rhs, blocks, agg, inverse, sol, res,
    lines_r, lines_w, coefs, factors, solved, sub_a, sub_c, sub_e, slab_a, slab_c, slab_e,
    inv_all, halo_0, halo_1, applied_0, onehot,
    block_here, block_split, inv_split, halo_split, block_sem,
    line_send, line_recv, coef_send, coef_recv, inv_send, inv_recv,
    sub_send, sub_recv, slab_send, slab_recv, halo_send, halo_recv,
):
    D, X, S, K, C = rhs.shape
    block_copy = pltpu.make_async_copy(blocks, block_here, block_sem)
    block_copy.start()
    slots = blocks.shape[3]
    aggregates = inv_all.shape[0] * inv_all.shape[1]
    slab, sub = lax.axis_index("slab"), lax.axis_index("sub")
    cells = [(x, s) for x in range(X) for s in range(S)]
    rows = [(d, x, s) for d in range(D) for x, s in cells]
    width = len(cells)

    barrier = pltpu.get_barrier_semaphore()
    for step in range(1, n_slab):
        pl.semaphore_signal(
            barrier, inc=1, device_id=(lax.rem(slab + step, n_slab), sub), device_id_type=MESH
        )
    for step in range(1, n_sub):
        pl.semaphore_signal(
            barrier, inc=1, device_id=(slab, lax.rem(sub + step, n_sub)), device_id_type=MESH
        )

    def copies(axis, buffer, send, recv, source=None):
        count, mine = (n_slab, slab) if axis == "slab" else (n_sub, sub)
        made = []
        for step in range(1, count):
            peer = lax.rem(mine + step, count)
            target = (peer, sub) if axis == "slab" else (slab, peer)
            made.append(
                pltpu.make_async_remote_copy(
                    src_ref=buffer.at[mine] if source is None else source,
                    dst_ref=buffer.at[mine],
                    send_sem=send.at[step],
                    recv_sem=recv.at[mine],
                    device_id=target,
                    device_id_type=MESH,
                )
            )
        for copy in made:
            copy.start()

        def wait():
            for step in range(1, count):
                peer = lax.rem(mine + step, count)
                pltpu.make_async_remote_copy(
                    src_ref=buffer.at[peer],
                    dst_ref=buffer.at[peer],
                    send_sem=send.at[step],
                    recv_sem=recv.at[peer],
                    device_id=(peer, sub) if axis == "slab" else (slab, peer),
                    device_id_type=MESH,
                ).wait_recv()
            for copy in made:
                copy.wait_send()

        return wait

    a_index = lax.broadcasted_iota(jnp.int32, (aggregates, C), 0)
    for n, (d, x, s) in enumerate(rows):
        onehot[:, pl.ds(n * C, C)] = (agg[d, x, s][None, :] == a_index).astype(F32).astype(BF16)

    def local_sums(read):
        split = jnp.concatenate([pieces(read(d, x, s), 3) for d, x, s in rows], axis=1)
        return stacked(dot(split, onehot[...], 1))

    slab_a[slab] = local_sums(lambda d, x, s: rhs[d, x, s])
    lines_r[slab] = rhs[...]
    inv_all[sub] = inverse[...]

    global_cross = X * n_sub
    plane_blocks = global_cross * S
    block_copy.wait()
    eye = (
        lax.broadcasted_iota(jnp.int32, (C, C), 0) == lax.broadcasted_iota(jnp.int32, (C, C), 1)
    ).astype(F32)
    for n, (d, x, s) in enumerate(rows):
        own = ((slab * D + d) * global_cross + sub * X + x) * S + s
        diagonal = jnp.zeros((C, C), F32)
        coupling = jnp.zeros((C, C), F32)
        for slot in range(slots):
            number = pattern[d, x, s, slot]
            block = block_here[d, x, s, slot]
            diagonal = diagonal + (number == own).astype(F32) * block
            coupling = coupling + (number == own - plane_blocks).astype(F32) * block
        coefs[slab, pl.ds(n, 1)] = jnp.sum(diagonal * eye, axis=0, keepdims=True)
        coefs[slab, pl.ds(len(rows) + n, 1)] = jnp.sum(coupling * eye, axis=0, keepdims=True)

    pl.semaphore_wait(barrier, n_slab + n_sub - 2)

    slab_wait = copies("slab", slab_a, slab_send.at[0], slab_recv.at[0])
    coefs_wait = copies("slab", coefs, coef_send, coef_recv)
    inv_wait = copies("sub", inv_all, inv_send, inv_recv, inverse)
    lines_wait = copies("slab", lines_r, line_send.at[0], line_recv.at[0], rhs)

    inv_wait()
    for other in range(n_sub):
        owned = inv_all.shape[1]
        part = inv_all[other]
        high = part.astype(BF16)
        inv_split[pl.ds(other * owned, owned)] = high
        inv_split[pl.ds((n_sub + other) * owned, owned)] = (part - high.astype(F32)).astype(BF16)

    def coarse_part(read):
        split = jnp.concatenate([pieces(read(layer), 3) for layer in range(n_slab)], axis=1)
        return joined(dot(split, inv_split[...], 1))

    def coarse_spread(values):
        return stacked(dot(pieces(values, 3), onehot[...], 0))

    def summed(buffer, count):
        total = buffer[0]
        for other in range(1, count):
            total = total + buffer[other]
        return total

    slab_wait()
    sub_a[sub] = coarse_part(lambda layer: slab_a[layer])
    sub_wait = copies("sub", sub_a, sub_send.at[0], sub_recv.at[0])

    coefs_wait()
    planes = n_slab * D

    def coef(kind, z):
        start = kind * len(rows) + (z % D) * width
        return coefs[z // D, pl.ds(start, width)]

    pivot = coef(0, 0)
    for z in range(planes):
        if z > 0:
            below = coef(1, z)
            pivot = coef(0, z) - below * below / pivot
        inverse_pivot = 1.0 / pivot
        factors[z, 0] = inverse_pivot
        factors[z, 1] = -coef(1, z) * inverse_pivot
        if z + 1 < planes:
            factors[z, 2] = -coef(1, z + 1) * inverse_pivot

    def line_solve(lines):
        carried = [None] * width
        for z in range(planes):
            for w, (x, s) in enumerate(cells):
                value = lines[z // D, z % D, x, s] * factors[z, 0, pl.ds(w, 1)]
                if z > 0:
                    value = value + factors[z, 1, pl.ds(w, 1)] * carried[w]
                carried[w] = value
                solved[z, x, s] = value
        for z in reversed(range(planes - 1)):
            for w, (x, s) in enumerate(cells):
                carried[w] = solved[z, x, s] + factors[z, 2, pl.ds(w, 1)] * carried[w]
                solved[z, x, s] = carried[w]

    for n, (d, x, s) in enumerate(rows):
        for slot in range(slots):
            block_split[n, :, pl.ds(slot * C, C)] = pieces(block_here[d, x, s, slot], 2)

    def exchange(halo, phase):
        def sides():
            inner_x, inner_z = pl.ds(1, X), pl.ds(1, D)
            return (
                (slab > 0, (slab - 1, sub), halo.at[1, inner_x], halo.at[D + 1, inner_x]),
                (slab < n_slab - 1, (slab + 1, sub), halo.at[D, inner_x], halo.at[0, inner_x]),
                (sub > 0, (slab, sub - 1), halo.at[inner_z, 1], halo.at[inner_z, X + 1]),
                (sub < n_sub - 1, (slab, sub + 1), halo.at[inner_z, X], halo.at[inner_z, 0]),
            )

        for side, (present, target, source, place) in enumerate(sides()):
            @pl.when(present)
            def _(side=side, target=target, source=source, place=place):
                pltpu.make_async_remote_copy(
                    src_ref=source, dst_ref=place,
                    send_sem=halo_send.at[phase, side], recv_sem=halo_recv.at[phase, side],
                    device_id=target, device_id_type=MESH,
                ).start()

        for side, (present, target, source, place) in enumerate(sides()):
            landing = sides()[side ^ 1][3]

            @pl.when(present)
            def _(side=side, target=target, source=source, landing=landing):
                pltpu.make_async_remote_copy(
                    src_ref=source, dst_ref=landing,
                    send_sem=halo_send.at[phase, side], recv_sem=halo_recv.at[phase, side ^ 1],
                    device_id=target, device_id_type=MESH,
                ).wait()

    def split_halo(halo):
        for d in range(D + 2):
            for x in range(X + 2):
                if 0 < d <= D or 0 < x <= X:
                    for s in range(S):
                        halo_split[d, x, s] = pieces(halo[d, x, s], 3)

    def apply_operator(n):
        d, x, s = rows[n]
        nearby = []
        for slot in range(slots):
            number = pattern[d, x, s, slot]
            remain = number % plane_blocks
            local_plane = jnp.clip(number // plane_blocks - slab * D + 1, 0, D + 1)
            local_cross = jnp.clip(remain // S - sub * X + 1, 0, X + 1)
            nearby.append(halo_split[local_plane, local_cross, remain % S])
        return joined(dot(jnp.concatenate(nearby, axis=1), block_split[n], 1))

    lane = lax.broadcasted_iota(jnp.int32, (K, C), 1)
    place = lax.broadcasted_iota(jnp.int32, (K, C), 0)

    def to_row(first, second):
        first = jnp.sum(first, axis=1, keepdims=True)
        second = jnp.sum(second, axis=1, keepdims=True)
        spread = jnp.where(lane == place, first, 0.0) + jnp.where(lane == place + K, second, 0.0)
        return jnp.sum(spread, axis=0, keepdims=True)

    def from_row(row):
        first = jnp.sum(jnp.where(lane == place, row, 0.0), axis=1, keepdims=True)
        second = jnp.sum(jnp.where(lane == place + K, row, 0.0), axis=1, keepdims=True)
        return first, second

    lines_wait()
    line_solve(lines_r)
    sub_wait()
    spread = coarse_spread(summed(sub_a, n_sub))
    for n, (d, x, s) in enumerate(rows):
        halo_0[d + 1, x + 1, s] = solved[slab * D + d, x, s] + spread[:, n * C : (n + 1) * C]

    exchange(halo_0, 0)
    split_halo(halo_0)
    energy = jnp.zeros((K, C), F32)
    curvature = jnp.zeros((K, C), F32)
    for n, (d, x, s) in enumerate(rows):
        applied = apply_operator(n)
        lines_w[slab, d, x, s] = applied
        applied_0[d, x, s] = applied
        smoothed = halo_0[d + 1, x + 1, s]
        energy = energy + rhs[d, x, s] * smoothed
        curvature = curvature + applied * smoothed

    slab_c[slab, pl.ds(0, K)] = local_sums(lambda d, x, s: applied_0[d, x, s])
    slab_c[slab, pl.ds(K, 1)] = to_row(energy, curvature)
    slab_wait = copies("slab", slab_c, slab_send.at[1], slab_recv.at[1])
    lines_wait = copies("slab", lines_w, line_send.at[1], line_recv.at[1])
    slab_wait()
    row = slab_c[0, pl.ds(K, 1)]
    for other in range(1, n_slab):
        row = row + slab_c[other, pl.ds(K, 1)]
    sub_c[sub, pl.ds(K, 1)] = row
    sub_c[sub, pl.ds(0, K)] = coarse_part(lambda layer: slab_c[layer, pl.ds(0, K)])
    sub_wait = copies("sub", sub_c, sub_send.at[1], sub_recv.at[1])
    lines_wait()
    line_solve(lines_w)
    sub_wait()
    total = summed(sub_c, n_sub)
    energy, curvature = from_row(total[K : K + 1])
    step_length = energy / curvature
    spread = coarse_spread(total[:K])
    for n, (d, x, s) in enumerate(rows):
        change = solved[slab * D + d, x, s] + spread[:, n * C : (n + 1) * C]
        halo_1[d + 1, x + 1, s] = halo_0[d + 1, x + 1, s] - step_length * change

    exchange(halo_1, 1)
    split_halo(halo_1)
    energy_sum = jnp.zeros((K, C), F32)
    curvature_sum = jnp.zeros((K, C), F32)
    for n, (d, x, s) in enumerate(rows):
        applied = apply_operator(n)
        sol[d, x, s] = applied
        smoothed = halo_1[d + 1, x + 1, s]
        residual = rhs[d, x, s] - step_length * applied_0[d, x, s]
        energy_sum = energy_sum + residual * smoothed
        curvature_sum = curvature_sum + applied * smoothed

    sub_e[sub] = to_row(energy_sum, curvature_sum)
    copies("sub", sub_e, sub_send.at[2], sub_recv.at[2])()
    row = sub_e[0]
    for other in range(1, n_sub):
        row = row + sub_e[other]
    slab_e[slab] = row
    copies("slab", slab_e, slab_send.at[2], slab_recv.at[2])()
    row = slab_e[0]
    for other in range(1, n_slab):
        row = row + slab_e[other]
    energy_next, curvature = from_row(row)
    growth = energy_next / energy
    step_next = energy_next / (curvature - growth * energy_next / step_length)
    for n, (d, x, s) in enumerate(rows):
        first, second = halo_0[d + 1, x + 1, s], halo_1[d + 1, x + 1, s]
        along_0, along_1 = applied_0[d, x, s], sol[d, x, s]
        residual = rhs[d, x, s] - step_length * along_0
        res[d, x, s] = residual - step_next * (along_1 + growth * along_0)
        sol[d, x, s] = step_length * first + step_next * (second + growth * first)


def hand_over(first_in, second_in, first_out, second_out):
    first_out[...] = first_in[...]
    second_out[...] = second_in[...]


def per_device(n_slab, n_sub, right_side, blocks, pattern, aggregates, coarse_inverse):
    D, X, S, K, C = right_side.shape
    owned, everything = coarse_inverse.shape
    layer = owned * n_sub
    planes = n_slab * D
    packed = -(-(K + 1) // 8) * 8
    rows = D * X * S
    field = (D, X, S, K, C)
    halo = (D + 2, X + 2, S, K, C)
    dma = pltpu.SemaphoreType.DMA
    vmem = pl.BlockSpec(memory_space=pltpu.VMEM)
    outputs = pl.pallas_call(
        functools.partial(kernel, n_slab, n_sub),
        out_shape=[jax.ShapeDtypeStruct(field, F32)] * 2,
        in_specs=[
            pl.BlockSpec(memory_space=pltpu.SMEM), vmem, pl.BlockSpec(memory_space=pl.ANY), vmem, vmem,
        ],
        out_specs=[vmem, vmem],
        scratch_shapes=[
            pltpu.VMEM((n_slab,) + field, F32),
            pltpu.VMEM((n_slab,) + field, F32),
            pltpu.VMEM((n_slab, 2 * rows, C), F32),
            pltpu.VMEM((planes, 3, X * S, C), F32),
            pltpu.VMEM((planes, X, S, K, C), F32),
            pltpu.VMEM((n_sub, K, layer), F32),
            pltpu.VMEM((n_sub, packed, layer), F32),
            pltpu.VMEM((n_sub, 1, C), F32),
            pltpu.VMEM((n_slab, K, layer), F32),
            pltpu.VMEM((n_slab, packed, layer), F32),
            pltpu.VMEM((n_slab, 1, C), F32),
            pltpu.VMEM((n_sub, owned, everything), F32),
            pltpu.VMEM(halo, F32),
            pltpu.VMEM(halo, F32),
            pltpu.VMEM(field, F32),
            pltpu.VMEM((layer, rows * C), BF16),
            pltpu.VMEM(blocks.shape, F32),
            pltpu.VMEM((rows, 2 * C, blocks.shape[3] * C), BF16),
            pltpu.VMEM((2 * layer, everything), BF16),
            pltpu.VMEM((D + 2, X + 2, S, 3 * K, C), BF16),
            dma,
            dma((2, n_slab)), dma((2, n_slab)),
            dma((n_slab,)), dma((n_slab,)),
            dma((n_sub,)), dma((n_sub,)),
            dma((3, n_sub)), dma((3, n_sub)),
            dma((3, n_slab)), dma((3, n_slab)),
            dma((2, 4)), dma((2, 4)),
        ],
        compiler_params=pltpu.CompilerParams(
            collective_id=0, has_side_effects=True, vmem_limit_bytes=60 * 1024 * 1024
        ),
        name="whole_solve",
    )(pattern, right_side, blocks, aggregates, coarse_inverse)
    return pl.pallas_call(
        hand_over,
        out_shape=[jax.ShapeDtypeStruct(field, F32)] * 2,
        in_specs=[vmem, vmem],
        out_specs=[vmem, vmem],
        compiler_params=pltpu.CompilerParams(vmem_limit_bytes=1024 * 1024),
        name="hand_over",
    )(*outputs)


def solution(mesh):
    placed = (
        P("slab", "sub", None, None, None),
        P("slab", "sub", None, None, None, None),
        P("slab", "sub", None, None),
        P("slab", "sub", None, None),
        P(("slab", "sub"), None),
    )
    body = functools.partial(per_device, mesh.shape["slab"], mesh.shape["sub"])
    return jax.shard_map(
        lambda *args: tuple(body(*args)),
        mesh=mesh,
        in_specs=placed,
        out_specs=(P("slab", "sub", None, None, None), P("slab", "sub", None, None, None)),
        check_vma=False,
    )
```
